256 devices in a mesh: depth: 2 (over x_hi), mode: 2 (over x_lo), tile: 64 (over z, y, core).
Axes of the slice: x: 4 (x_hi: 2, x_lo: 2; x = x_hi * 2 + x_lo), y: 4, z: 8, core: 2. Of those that a mesh axis runs over, the one named last changes fastest.
Arguments:
- probe: float32 [2, 2, 256, 256], P('mode'), may hold values from -3 to 3
- object_slices: float32 [2, 2, 384, 16384], P('depth', None, None, 'tile'), may hold values from -4.2 to 4.2
- positions: int32 [128, 2], P('tile'), may hold values from 0 to 256, as said below
- measured: float32 [128, 256, 256], P('tile'), may hold values from 0 to 2
Outputs:
- object_gradient: float32 [2, 2, 384, 16384], P('depth', None, None, 'tile')
The draws below stay inside these ranges and needn't reach their ends.
Inputs may be any that keep to these rules, and one draw needn't show every extreme that they name: `positions`: position r belongs to tile r // 2. Entry 0 is its window's first row, at most 128; entry 1 is its first column counted in the tile's columns extended by 128 on each side, at most 256. Windows never leave the object: in the first tile the column entry is at least 128, in the last at most 128.
All inputs are finite; a program needn't handle non-finite values.
Results may differ from the reference program's by a relative error of at most 0.0003.
Values sent between devices are 32-bit elements; how exact they have to be, the bound alone decides.
No kernel may reach another device: no remote copies, remote signals or barrier semaphores. Data moves between devices by JAX's collectives and lax.ppermute only.
A program may use at most 64 MiB of HBM per device.

```python
import math
import jax
import jax.numpy as jnp
from jax import lax

PROBE = 256
HALO = 128
TILE_X = 256
TILE_Y = 384
POS_DEV = 2
MODES = 2
SLICES = 2
POSITIONS = 128
OBJ_X = 16384


def draw_positions(key, part):
    count = POSITIONS
    tiles = POSITIONS // POS_DEV
    rows = jnp.arange(count, dtype=jnp.int32)
    owner = rows // POS_DEV
    lowest = jnp.where(owner == 0, HALO, 0)
    highest_col = jnp.where(owner == tiles - 1, HALO + TILE_X - PROBE, TILE_X + 2 * HALO - PROBE)
    key_rows = jax.random.fold_in(key, 11)
    key_cols = jax.random.fold_in(key, 23)
    top = jax.random.randint(key_rows, (count,), 0, TILE_Y - PROBE + 1, dtype=jnp.int32)
    spread = jax.random.randint(key_cols, (count,), 0, 1 << 20, dtype=jnp.int32)
    left = lowest + spread % (highest_col - lowest + 1)
    return jnp.stack([top, left], 1).astype(jnp.int32)


def block_scale(stream_key, dims, cuts, least, top_value):
    def one(dim, parts):
        heights = jax.random.uniform(jax.random.fold_in(jax.random.fold_in(stream_key, 6), dim), (parts,), jnp.float32, least / len(cuts), top_value / len(cuts))
        return jnp.repeat(jnp.exp(heights), dims[dim] // parts).reshape((-1,) + (1,) * (len(dims) - dim - 1))

    level = one(*cuts[0])
    for cut in cuts[1:]:
        level = level * one(*cut)
    return level


def bell_draw(own_key, extent, deviation, limit, split=(), kind=jnp.bfloat16):
    values = deviation * jax.random.normal(own_key, extent, jnp.float32)
    if split:
        values = values * block_scale(own_key, extent, split, -0.22, 0.18)
    return jnp.clip(values, -limit, limit).astype(kind)


def setup_inputs(seed: int = 0) -> dict:
    seeds = jax.random.split(jax.random.key(seed), 5)
    probe = bell_draw(seeds[0], (MODES, 2, PROBE, PROBE), 0.5, 3.0, ((0, 2),), jnp.float32)
    object_slices = bell_draw(seeds[1], (SLICES, 2, TILE_Y, OBJ_X), 0.7, 4.2, ((0, 2), (3, 64)), jnp.float32)
    positions = draw_positions(jax.random.fold_in(seeds[4], 71), 0)
    measured = jnp.clip(2.0 * jax.random.uniform(seeds[3], (POSITIONS, PROBE, PROBE), jnp.float32) ** block_scale(seeds[3], (POSITIONS, PROBE, PROBE), ((0, 64),), -0.2, 0.2), 0.0, 2.0)
    return {"probe": probe, "object_slices": object_slices, "positions": positions, "measured": measured}


def propagator(length):
    ordinal = jnp.arange(length, dtype=jnp.int32)
    signed = jnp.where(ordinal < length - length // 2, ordinal, ordinal - length)
    square = signed[:, None] * signed[:, None] + signed[None, :] * signed[None, :]
    angle = (-math.pi / (2.0 * length)) * ((3 * square) % (4 * length)).astype(jnp.float32)
    return lax.complex(jnp.cos(angle), jnp.sin(angle))


def reference(probe, object_slices, positions, measured):
    length = PROBE
    slices = object_slices.shape[0]
    transfer = propagator(length)
    extended = lax.complex(object_slices[:, 0], object_slices[:, 1])
    extended = jnp.pad(extended, ((0, 0), (0, 0), (HALO, HALO)))
    start_wave = lax.complex(probe[:, 0], probe[:, 1])
    zeros_real = jnp.zeros(extended.shape, jnp.float32)

    def visit(carry, entry):
        accum_r, accum_i = carry
        row_index, offset, pattern = entry
        owner = (row_index // POS_DEV).astype(jnp.int32)
        top = offset[0].astype(jnp.int32)
        column = (owner * TILE_X + offset[1]).astype(jnp.int32)
        start = (jnp.zeros((), jnp.int32), top, column)
        window = lax.dynamic_slice(extended, start, (slices, length, length))
        wave = start_wave
        inputs = []
        result = wave
        for layer_no in range(slices):
            inputs.append(wave)
            moved = wave * window[layer_no]
            result = jnp.fft.fft2(moved, norm="ortho")
            if layer_no + 1 < slices:
                wave = jnp.fft.ifft2(result * transfer, norm="ortho")
        intensity = jnp.sum(result.real * result.real + result.imag * result.imag, axis=0)
        grad = (intensity - pattern)[None] * result
        pieces = [None] * slices
        for layer_no in reversed(range(slices)):
            if layer_no == slices - 1:
                inner = jnp.fft.ifft2(grad, norm="ortho")
            else:
                inner = jnp.fft.ifft2(jnp.conj(transfer) * jnp.fft.fft2(grad, norm="ortho"), norm="ortho")
            pieces[layer_no] = jnp.sum(jnp.conj(inputs[layer_no]) * inner, axis=0)
            grad = jnp.conj(window[layer_no])[None] * inner
        stacked = jnp.stack(pieces, 0)
        current_r = lax.dynamic_slice(accum_r, start, (slices, length, length))
        current_i = lax.dynamic_slice(accum_i, start, (slices, length, length))
        accum_r = lax.dynamic_update_slice(accum_r, current_r + stacked.real, start)
        accum_i = lax.dynamic_update_slice(accum_i, current_i + stacked.imag, start)
        return (accum_r, accum_i), None

    rows = jnp.arange(positions.shape[0], dtype=jnp.int32)
    (accum_r, accum_i), unused = lax.scan(visit, (zeros_real, zeros_real), (rows, positions, measured))
    width = accum_r.shape[2] - 2 * HALO
    core_r = accum_r[:, :, HALO:HALO + width]
    core_i = accum_i[:, :, HALO:HALO + width]
    return jnp.stack([core_r, core_i], 1)
```

```python
import numpy as np

import jax
import jax.numpy as jnp
from jax import lax
from jax.experimental import pallas as pl
from jax.experimental.pallas import tpu as pltpu
from jax.sharding import PartitionSpec as P

HALF = 128
FULL = 256
ROWS = 384
F32 = jnp.float32
BF16 = jnp.bfloat16
FS, FT, GS, GT, MS, MT, CS, CT = range(8)


def tables():
    n = np.arange(HALF)
    unit = lambda k: np.exp(-2j * np.pi * (k % FULL) / FULL) / 16.0
    even = unit(2 * n[:, None] * n[None, :])
    odd = unit(n[:, None] * (2 * n[None, :] + 1))
    j = np.arange(FULL)
    dft = unit(j[:, None] * j[None, :])
    f = np.where(j < HALF, j, j - FULL)
    h = np.exp(-2j * np.pi * (3 * f * f % 1024) / 1024)
    prop = dft.conj() @ (h[:, None] * dft)
    near, far = prop[:HALF, :HALF], prop[:HALF, HALF:]
    ms, mt = (near + far) / 2, (near - far) / 2
    pairs = lambda c: np.block([[c.real, c.imag], [-c.imag, c.real]])
    mats = [even, odd, even.conj(), odd.conj().T, ms, mt, ms.conj(), mt.conj()]
    whole = np.stack([pairs(c) for c in mats]).astype(np.float32)
    high = whole.astype(jnp.bfloat16)
    low = (whole - high.astype(np.float32)).astype(jnp.bfloat16)
    src = np.concatenate([np.arange(0, FULL, 2), np.arange(1, FULL, 2)])
    sort = np.zeros((FULL, FULL), np.float32)
    sort[src, np.arange(FULL)] = 1.0
    return high, low, sort.astype(jnp.bfloat16)


def split(x):
    high = x.astype(BF16)
    return high, (x - high.astype(F32)).astype(BF16)


def dot(a, b):
    return jnp.dot(a, b, preferred_element_type=F32)


RC = 32


def kernel(info, own_o, own_i, own_on, own_in, oth_o, oth_i, oth_on, oth_in, prb0, prb1,
           meas, kh, kl, sort, g_o, g_i, g_on, g_in,
           ext, acc, win, psi, lh, rh, mo, fld, mp, cols):
    d = info[4]
    odd = info[5]
    for blk, own, oth in ((0, own_on, oth_on), (1, own_o, oth_o), (2, own_i, oth_i), (3, own_in, oth_in)):
        at = blk + odd * (3 - 2 * blk)
        ext[d, at] = own[...]
        ext[1 - d, at] = oth[...]
    acc[...] = jnp.zeros(acc.shape, F32)
    lane = lax.broadcasted_iota(jnp.int32, (RC, HALF), 1)
    probes = (prb0, prb1)

    def put(ref, k, mode, rows, cols, value):
        high, low = split(value)
        ref[0, k, mode, rows, cols] = high
        ref[1, k, mode, rows, cols] = low

    def right(ks, kt):
        for mode in range(2):
            for k, kk in ((0, ks), (1, kt)):
                for r in range(0, FULL, HALF):
                    rr = pl.ds(r, HALF)
                    xh, xl = lh[0, k, mode, rr], lh[1, k, mode, rr]
                    mo[k, mode, rr] = dot(xh, kh[kk]) + (dot(xh, kl[kk]) + dot(xl, kh[kk]))

    def left(ks, kt, dst):
        for mode in range(2):
            for k, kk in ((0, ks), (1, kt)):
                for r in range(0, FULL, HALF):
                    rr = pl.ds(r, HALF)
                    ch, cl = kh[kk, rr], kl[kk, rr]
                    xh, xl = rh[0, k, mode], rh[1, k, mode]
                    dst[k, mode, rr] = dot(ch, xh) + (dot(cl, xh) + dot(ch, xl))

    def halves_to_lh(mode, r, ur, ui):
        rows = pl.ds(r, RC)
        a, b = ur[:, :HALF], ur[:, HALF:]
        c, e = ui[:, :HALF], ui[:, HALF:]
        put(lh, 0, mode, rows, pl.ds(0, HALF), a + b)
        put(lh, 1, mode, rows, pl.ds(0, HALF), a - b)
        put(lh, 0, mode, rows, pl.ds(HALF, HALF), c + e)
        put(lh, 1, mode, rows, pl.ds(HALF, HALF), c - e)

    def prop_middle():
        for mode in range(2):
            for r in range(0, HALF, RC):
                top, bot = pl.ds(r, RC), pl.ds(HALF + r, RC)
                pt, qt = mo[0, mode, top], mo[1, mode, top]
                pb, qb = mo[0, mode, bot], mo[1, mode, bot]
                for sign, k in ((1, 0), (-1, 1)):
                    p = pt + pb if sign > 0 else pt - pb
                    q = qt + qb if sign > 0 else qt - qb
                    y0, y1 = p + q, p - q
                    put(rh, k, mode, top, pl.ds(0, HALF), y0[:, :HALF])
                    put(rh, k, mode, top, pl.ds(HALF, HALF), y1[:, :HALF])
                    put(rh, k, mode, bot, pl.ds(0, HALF), y0[:, HALF:])
                    put(rh, k, mode, bot, pl.ds(HALF, HALF), y1[:, HALF:])

    def natural(src, mode, r):
        base = r % HALF
        top, bot = pl.ds(base, RC), pl.ds(HALF + base, RC)
        if r < HALF:
            return src[0, mode, top] + src[1, mode, top], src[0, mode, bot] + src[1, mode, bot]
        return src[0, mode, top] - src[1, mode, top], src[0, mode, bot] - src[1, mode, bot]

    def position(pos, carry):
        top = info[2 * pos]
        col = info[2 * pos + 1]
        q = jnp.where(col >= HALF, 1, 0)
        shift = col - q * HALF
        back = jnp.where(shift == 0, 0, HALF - shift)
        fwd = jnp.where(shift == HALF, 0, shift)
        keep = lane < HALF - shift
        for s in range(2):
            for c in range(2):
                for r in range(0, FULL, RC):
                    rot = [pltpu.roll(ext[s, q + b, c, pl.ds(top + r, RC), :], back, axis=1) for b in range(3)]
                    win[s, c, pl.ds(r, RC), pl.ds(0, HALF)] = jnp.where(keep, rot[0], rot[1])
                    win[s, c, pl.ds(r, RC), pl.ds(HALF, HALF)] = jnp.where(keep, rot[1], rot[2])
        for c in range(2):
            cols[c] = meas[pos, :, pl.ds(c * HALF, HALF)]
        for par in range(2):
            m = jnp.concatenate([cols[c, pl.ds(par, HALF, stride=2), :] for c in range(2)], axis=1)
            m1 = m.astype(BF16)
            rest = m - m1.astype(F32)
            m2 = rest.astype(BF16)
            m3 = (rest - m2.astype(F32)).astype(BF16)
            mp[par] = dot(m1, sort[...]) + (dot(m2, sort[...]) + dot(m3, sort[...]))
        for mode in range(2):
            for r in range(0, FULL, RC):
                rr = pl.ds(r, RC)
                pr, pi = probes[mode][0, rr], probes[mode][1, rr]
                wr, wi = win[0, 0, rr], win[0, 1, rr]
                halves_to_lh(mode, r, pr * wr - pi * wi, pr * wi + pi * wr)
        right(MS, MT)
        prop_middle()
        left(CS, CT, fld)
        for mode in range(2):
            for r in range(0, FULL, RC):
                rr = pl.ds(r, RC)
                pr, pi = natural(fld, mode, r)
                psi[mode, 0, rr] = pr
                psi[mode, 1, rr] = pi
                wr, wi = win[1, 0, rr], win[1, 1, rr]
                halves_to_lh(mode, r, pr * wr - pi * wi, pr * wi + pi * wr)
        right(FS, FT)
        for mode in range(2):
            for r in range(0, HALF, RC):
                tp, bt = pl.ds(r, RC), pl.ds(HALF + r, RC)
                for c in range(2):
                    et, eb = mo[c, mode, tp], mo[c, mode, bt]
                    s, t = et + eb, et - eb
                    at = pl.ds(c * HALF, HALF)
                    put(rh, 0, mode, tp, at, s[:, :HALF])
                    put(rh, 0, mode, bt, at, s[:, HALF:])
                    put(rh, 1, mode, tp, at, t[:, :HALF])
                    put(rh, 1, mode, bt, at, t[:, HALF:])
        left(GS, GT, fld)
        for par in range(2):
            for r in range(0, HALF, RC):
                tp, bt = pl.ds(r, RC), pl.ds(HALF + r, RC)
                fr = [fld[par, mode, tp] for mode in range(2)]
                fi = [fld[par, mode, bt] for mode in range(2)]
                resid = (fr[0] * fr[0] + fi[0] * fi[0]) + (fr[1] * fr[1] + fi[1] * fi[1]) - mp[par, tp]
                for mode in range(2):
                    put(rh, par, mode, tp, slice(None), resid * fr[mode])
                    put(rh, par, mode, bt, slice(None), resid * fi[mode])
        left(FS, FT, fld)
        for mode in range(2):
            for r in range(0, FULL, RC):
                rr = pl.ds(r, RC)
                xr, xi = natural(fld, mode, r)
                put(lh, 0, mode, rr, pl.ds(0, HALF), xr[:, :HALF])
                put(lh, 0, mode, rr, pl.ds(HALF, HALF), xi[:, :HALF])
                put(lh, 1, mode, rr, pl.ds(0, HALF), xr[:, HALF:])
                put(lh, 1, mode, rr, pl.ds(HALF, HALF), xi[:, HALF:])
        right(GS, GT)

        def wave_back(mode, rr):
            p, q_ = mo[0, mode, rr], mo[1, mode, rr]
            y0, y1 = p + q_, p - q_
            qr = jnp.concatenate([y0[:, :HALF], y1[:, :HALF]], axis=1)
            qi = jnp.concatenate([y0[:, HALF:], y1[:, HALF:]], axis=1)
            return qr, qi

        @pl.when(d == 0)
        def _():
            for mode in range(2):
                for r in range(0, FULL, RC):
                    rr = pl.ds(r, RC)
                    qr, qi = wave_back(mode, rr)
                    wr, wi = win[1, 0, rr], win[1, 1, rr]
                    halves_to_lh(mode, r, wr * qr + wi * qi, wr * qi - wi * qr)
            right(CS, CT)
            prop_middle()
            left(MS, MT, fld)
            for r in range(0, FULL, RC):
                rr = pl.ds(r, RC)
                vr = vi = None
                for mode in range(2):
                    qr, qi = natural(fld, mode, r)
                    pr, pi = probes[mode][0, rr], probes[mode][1, rr]
                    ar, ai = pr * qr + pi * qi, pr * qi - pi * qr
                    vr, vi = (ar, ai) if vr is None else (vr + ar, vi + ai)
                win[0, 0, rr] = vr
                win[0, 1, rr] = vi

        @pl.when(d != 0)
        def _():
            for r in range(0, FULL, RC):
                rr = pl.ds(r, RC)
                vr = vi = None
                for mode in range(2):
                    qr, qi = wave_back(mode, rr)
                    pr, pi = psi[mode, 0, rr], psi[mode, 1, rr]
                    ar, ai = pr * qr + pi * qi, pr * qi - pi * qr
                    vr, vi = (ar, ai) if vr is None else (vr + ar, vi + ai)
                win[0, 0, rr] = vr
                win[0, 1, rr] = vi

        later = lane >= shift
        zero = jnp.zeros((RC, HALF), F32)
        for c in range(2):
            for r in range(0, FULL, RC):
                rr = pl.ds(r, RC)
                r0 = pltpu.roll(win[0, c, rr, pl.ds(0, HALF)], fwd, axis=1)
                r1 = pltpu.roll(win[0, c, rr, pl.ds(HALF, HALF)], fwd, axis=1)
                vals = (jnp.where(later, r0, zero), jnp.where(later, r1, r0), jnp.where(later, zero, r1))
                for b in range(3):
                    acc[q + b, c, pl.ds(top + r, RC), :] = acc[q + b, c, pl.ds(top + r, RC), :] + vals[b]
        return carry

    lax.fori_loop(0, 2, position, 0)
    for blk, out in ((0, g_on), (1, g_o), (2, g_i), (3, g_in)):
        out[...] = acc[blk + odd * (3 - 2 * blk)]


def merge(flag, a, b, ra, rb, out):
    odd = flag[5]
    out[0, :, :, pl.ds(pl.multiple_of(odd * HALF, HALF), HALF)] = a[...] + ra[...]
    out[0, :, :, pl.ds(pl.multiple_of((1 - odd) * HALF, HALF), HALF)] = b[...] + rb[...]


def body(probe, object_slices, positions, measured):
    d = lax.axis_index("depth")
    m = lax.axis_index("mode")
    t = lax.axis_index("tile")
    tiles = lax.axis_size("tile")
    odd = t % 2
    cross = [(0, 3), (3, 0), (1, 2), (2, 1)]
    pair = [(i, i ^ 1) for i in range(tiles)]
    side = [(i, i + 1) for i in range(1, tiles - 1, 2)]
    side = side + [(j, i) for i, j in side]
    o = object_slices[0]
    lft, rgt = o[..., :HALF], o[..., HALF:]
    own_o = jnp.where(odd == 0, lft, rgt)
    own_i = jnp.where(odd == 0, rgt, lft)
    oth_o = lax.ppermute(own_o, ("depth", "mode"), cross)
    oth_i = lax.ppermute(own_i, ("depth", "mode"), cross)
    own_on = lax.ppermute(own_o, "tile", side)
    own_in = lax.ppermute(own_i, "tile", pair)
    prb = lax.ppermute(probe, "mode", [(0, 1), (1, 0)])
    oth_on = lax.ppermute(oth_o, "tile", side)
    oth_in = lax.ppermute(oth_i, "tile", pair)
    info = jnp.concatenate([positions.reshape(-1), jnp.stack([d, odd]).astype(jnp.int32)])
    high, low, sort = tables()
    blk = jax.ShapeDtypeStruct((2, ROWS, HALF), F32)
    smem = pl.BlockSpec(memory_space=pltpu.SMEM)
    vmem = pl.BlockSpec(memory_space=pltpu.VMEM)
    g_o, g_i, g_on, g_in = pl.pallas_call(
        kernel,
        out_shape=(blk,) * 4,
        in_specs=[smem] + [vmem] * 14,
        out_specs=(vmem,) * 4,
        scratch_shapes=[
            pltpu.VMEM((2, 4, 2, ROWS, HALF), F32),
            pltpu.VMEM((4, 2, ROWS, HALF), F32),
            pltpu.VMEM((2, 2, FULL, FULL), F32),
            pltpu.VMEM((2, 2, FULL, FULL), F32),
            pltpu.VMEM((2, 2, 2, FULL, FULL), BF16),
            pltpu.VMEM((2, 2, 2, FULL, FULL), BF16),
            pltpu.VMEM((2, 2, FULL, FULL), F32),
            pltpu.VMEM((2, 2, FULL, FULL), F32),
            pltpu.VMEM((2, HALF, FULL), F32),
            pltpu.VMEM((2, FULL, HALF), F32),
        ],
        name="grad",
    )(info, own_o, own_i, own_on, own_in, oth_o, oth_i, oth_on, oth_in, probe[0], prb[0],
      measured, jnp.asarray(high), jnp.asarray(low), jnp.asarray(sort))
    r_o = lax.ppermute(g_on, "tile", side)
    r_i = lax.ppermute(g_in, "tile", pair)
    return pl.pallas_call(
        merge,
        out_shape=jax.ShapeDtypeStruct((1, 2, ROWS, FULL), F32),
        in_specs=[smem] + [vmem] * 4,
        out_specs=vmem,
        name="merge",
    )(info, g_o, g_i, r_o, r_i)


def solution(mesh):
    placed = (
        P("mode", None, None, None),
        P("depth", None, None, "tile"),
        P("tile", None),
        P("tile", None, None),
    )
    return jax.shard_map(
        body, mesh=mesh, in_specs=placed, out_specs=P("depth", None, None, "tile"), check_vma=False
    )
```

```python
import numpy as np

import jax
import jax.numpy as jnp
from jax import lax
from jax.experimental import pallas as pl
from jax.experimental.pallas import tpu as pltpu
from jax.sharding import PartitionSpec as P


HALF = 128
FULL = 256
ROWS = 384
F32 = jnp.float32
BF16 = jnp.bfloat16
FS, FT, GS, GT, MS, MT, CS, CT = range(8)


def tables():
    n = np.arange(HALF)
    unit = lambda k: np.exp(-2j * np.pi * (k % FULL) / FULL) / 16.0
    even = unit(2 * n[:, None] * n[None, :])
    odd = unit(n[:, None] * (2 * n[None, :] + 1))
    j = np.arange(FULL)
    dft = unit(j[:, None] * j[None, :])
    f = np.where(j < HALF, j, j - FULL)
    h = np.exp(-2j * np.pi * (3 * f * f % 1024) / 1024)
    prop = dft.conj() @ (h[:, None] * dft)
    near, far = prop[:HALF, :HALF], prop[:HALF, HALF:]
    ms, mt = (near + far) / 2, (near - far) / 2
    pairs = lambda c: np.block([[c.real, c.imag], [-c.imag, c.real]])
    mats = [even, odd, even.conj(), odd.conj().T, ms, mt, ms.conj(), mt.conj()]
    whole = np.stack([pairs(c) for c in mats]).astype(np.float32)
    high = whole.astype(jnp.bfloat16)
    low = (whole - high.astype(np.float32)).astype(jnp.bfloat16)
    src = np.concatenate([np.arange(0, FULL, 2), np.arange(1, FULL, 2)])
    sort = np.zeros((FULL, FULL), np.float32)
    sort[src, np.arange(FULL)] = 1.0
    return high, low, sort.astype(jnp.bfloat16)


def split(x):
    high = x.astype(BF16)
    return high, (x - high.astype(F32)).astype(BF16)


def dot(a, b):
    return jnp.dot(a, b, preferred_element_type=F32)


RC = 32
LIMIT = 20 * 2**20


def put(ref, k, mode, rows, cols, value):
    high, low = split(value)
    ref[0, k, mode, rows, cols] = high
    ref[1, k, mode, rows, cols] = low


def right(lh, mo, kh, kl, ks, kt):
    for mode in range(2):
        for k, kk in ((0, ks), (1, kt)):
            for r in range(0, FULL, HALF):
                rr = pl.ds(r, HALF)
                xh, xl = lh[0, k, mode, rr], lh[1, k, mode, rr]
                mo[k, mode, rr] = dot(xh, kh[kk]) + (dot(xh, kl[kk]) + dot(xl, kh[kk]))


def left(rh, dst, kh, kl, ks, kt):
    for mode in range(2):
        for k, kk in ((0, ks), (1, kt)):
            for r in range(0, FULL, HALF):
                rr = pl.ds(r, HALF)
                ch, cl = kh[kk, rr], kl[kk, rr]
                xh, xl = rh[0, k, mode], rh[1, k, mode]
                dst[k, mode, rr] = dot(ch, xh) + (dot(cl, xh) + dot(ch, xl))


def halves_to_lh(lh, mode, r, ur, ui):
    rows = pl.ds(r, RC)
    a, b = ur[:, :HALF], ur[:, HALF:]
    c, e = ui[:, :HALF], ui[:, HALF:]
    put(lh, 0, mode, rows, pl.ds(0, HALF), a + b)
    put(lh, 1, mode, rows, pl.ds(0, HALF), a - b)
    put(lh, 0, mode, rows, pl.ds(HALF, HALF), c + e)
    put(lh, 1, mode, rows, pl.ds(HALF, HALF), c - e)


def prop_middle(mo, rh):
    for mode in range(2):
        for r in range(0, HALF, RC):
            top, bot = pl.ds(r, RC), pl.ds(HALF + r, RC)
            pt, qt = mo[0, mode, top], mo[1, mode, top]
            pb, qb = mo[0, mode, bot], mo[1, mode, bot]
            for sign, k in ((1, 0), (-1, 1)):
                p = pt + pb if sign > 0 else pt - pb
                q = qt + qb if sign > 0 else qt - qb
                y0, y1 = p + q, p - q
                put(rh, k, mode, top, pl.ds(0, HALF), y0[:, :HALF])
                put(rh, k, mode, top, pl.ds(HALF, HALF), y1[:, :HALF])
                put(rh, k, mode, bot, pl.ds(0, HALF), y0[:, HALF:])
                put(rh, k, mode, bot, pl.ds(HALF, HALF), y1[:, HALF:])


def natural(src, mode, r):
    base = r % HALF
    top, bot = pl.ds(base, RC), pl.ds(HALF + base, RC)
    if r < HALF:
        return src[0, mode, top] + src[1, mode, top], src[0, mode, bot] + src[1, mode, bot]
    return src[0, mode, top] - src[1, mode, top], src[0, mode, bot] - src[1, mode, bot]


def place(info, pos):
    top = info[pos, 0]
    col = info[pos, 1]
    q = jnp.where(col >= HALF, 1, 0)
    return top, q, col - q * HALF


def gather(odd, parts, ext):
    outer, inner, far_outer, far_inner = parts
    for blk, src in ((0, far_outer), (1, outer), (2, inner), (3, far_inner)):
        ext[blk + odd * (3 - 2 * blk)] = src[...]


def cut(info, pos, ext, store):
    top, q, shift = place(info, pos)
    lane = lax.broadcasted_iota(jnp.int32, (RC, HALF), 1)
    back = jnp.where(shift == 0, 0, HALF - shift)
    keep = lane < HALF - shift
    for c in range(2):
        for r in range(0, FULL, RC):
            rot = [pltpu.roll(ext[q + b, c, pl.ds(top + r, RC), :], back, axis=1) for b in range(3)]
            store(c, pl.ds(r, RC), pl.ds(0, HALF), jnp.where(keep, rot[0], rot[1]))
            store(c, pl.ds(r, RC), pl.ds(HALF, HALF), jnp.where(keep, rot[1], rot[2]))


def halve(whole, outer, inner, sem):
    odd = lax.axis_index("tile") % 2
    copies = []
    for k, (side, half) in enumerate(((odd, outer), (1 - odd, inner))):
        lanes = pl.ds(pl.multiple_of(side * HALF, HALF), HALF)
        copies.append(pltpu.make_async_copy(whole.at[0, :, :, lanes], half, sem.at[k]))
        copies[-1].start()
    for copy in copies:
        copy.wait()


def early(info, own_o, own_i, own_on, own_in, prb_hbm, prb1, meas_hbm, kh_hbm, kl_hbm, sort_hbm,
          wown, psi, mp, kh, kl, prb0, ext, lh, rh, mo, fld, cols, meas, sort, sem):
    d = lax.axis_index("depth")
    moves = [(kh_hbm, kh), (kl_hbm, kl), (prb_hbm.at[0], prb0), (meas_hbm, meas), (sort_hbm, sort)]
    copies = [pltpu.make_async_copy(src, dst, sem.at[k]) for k, (src, dst) in enumerate(moves)]
    for copy in copies:
        copy.start()
    gather(lax.axis_index("tile") % 2, (own_o, own_i, own_on, own_in), ext)
    for copy in copies:
        copy.wait()
    probes = (prb0, prb1)

    def position(pos, carry):
        def store(c, rows, at, value):
            wown[pos, c, rows, at] = value

        cut(info, pos, ext, store)
        for c in range(2):
            cols[c] = meas[pos, :, pl.ds(c * HALF, HALF)]
        for par in range(2):
            m = jnp.concatenate([cols[c, pl.ds(par, HALF, stride=2), :] for c in range(2)], axis=1)
            m1 = m.astype(BF16)
            rest = m - m1.astype(F32)
            m2 = rest.astype(BF16)
            m3 = (rest - m2.astype(F32)).astype(BF16)
            mp[pos, par] = dot(m1, sort[...]) + (dot(m2, sort[...]) + dot(m3, sort[...]))

        @pl.when(d == 0)
        def _():
            for mode in range(2):
                for r in range(0, FULL, RC):
                    rr = pl.ds(r, RC)
                    pr, pi = probes[mode][0, rr], probes[mode][1, rr]
                    wr, wi = wown[pos, 0, rr], wown[pos, 1, rr]
                    halves_to_lh(lh, mode, r, pr * wr - pi * wi, pr * wi + pi * wr)
            right(lh, mo, kh, kl, MS, MT)
            prop_middle(mo, rh)
            left(rh, fld, kh, kl, CS, CT)
            for mode in range(2):
                for r in range(0, FULL, RC):
                    pr, pi = natural(fld, mode, r)
                    psi[pos, mode, 0, pl.ds(r, RC)] = pr
                    psi[pos, mode, 1, pl.ds(r, RC)] = pi

        return carry

    lax.fori_loop(0, 2, position, 0)


def grad(info, oth_o, oth_i, oth_on, oth_in, wown, psi0, mp, prb0, prb1, kh, kl, g_o, g_i, g_on, g_in,
         ext, acc, win, psi, lh, rh, mo, fld):
    d = lax.axis_index("depth")
    odd = lax.axis_index("tile") % 2
    gather(odd, (oth_o, oth_i, oth_on, oth_in), ext)
    acc[...] = jnp.zeros(acc.shape, F32)
    probes = (prb0, prb1)

    def position(pos, carry):
        def store(c, rows, at, value):
            win[c, rows, at] = value

        cut(info, pos, ext, store)

        @pl.when(d == 0)
        def _():
            for mode in range(2):
                for r in range(0, FULL, RC):
                    rr = pl.ds(r, RC)
                    pr, pi = psi0[pos, mode, 0, rr], psi0[pos, mode, 1, rr]
                    wr, wi = win[0, rr], win[1, rr]
                    halves_to_lh(lh, mode, r, pr * wr - pi * wi, pr * wi + pi * wr)

        @pl.when(d != 0)
        def _():
            for mode in range(2):
                for r in range(0, FULL, RC):
                    rr = pl.ds(r, RC)
                    pr, pi = probes[mode][0, rr], probes[mode][1, rr]
                    wr, wi = win[0, rr], win[1, rr]
                    halves_to_lh(lh, mode, r, pr * wr - pi * wi, pr * wi + pi * wr)
            right(lh, mo, kh, kl, MS, MT)
            prop_middle(mo, rh)
            left(rh, fld, kh, kl, CS, CT)
            for mode in range(2):
                for r in range(0, FULL, RC):
                    rr = pl.ds(r, RC)
                    pr, pi = natural(fld, mode, r)
                    psi[mode, 0, rr] = pr
                    psi[mode, 1, rr] = pi
                    wr, wi = wown[pos, 0, rr], wown[pos, 1, rr]
                    halves_to_lh(lh, mode, r, pr * wr - pi * wi, pr * wi + pi * wr)

        right(lh, mo, kh, kl, FS, FT)
        for mode in range(2):
            for r in range(0, HALF, RC):
                tp, bt = pl.ds(r, RC), pl.ds(HALF + r, RC)
                for c in range(2):
                    et, eb = mo[c, mode, tp], mo[c, mode, bt]
                    s, t = et + eb, et - eb
                    at = pl.ds(c * HALF, HALF)
                    put(rh, 0, mode, tp, at, s[:, :HALF])
                    put(rh, 0, mode, bt, at, s[:, HALF:])
                    put(rh, 1, mode, tp, at, t[:, :HALF])
                    put(rh, 1, mode, bt, at, t[:, HALF:])
        left(rh, fld, kh, kl, GS, GT)
        for par in range(2):
            for r in range(0, HALF, RC):
                tp, bt = pl.ds(r, RC), pl.ds(HALF + r, RC)
                fr = [fld[par, mode, tp] for mode in range(2)]
                fi = [fld[par, mode, bt] for mode in range(2)]
                resid = (fr[0] * fr[0] + fi[0] * fi[0]) + (fr[1] * fr[1] + fi[1] * fi[1]) - mp[pos, par, tp]
                for mode in range(2):
                    put(rh, par, mode, tp, slice(None), resid * fr[mode])
                    put(rh, par, mode, bt, slice(None), resid * fi[mode])
        left(rh, fld, kh, kl, FS, FT)
        for mode in range(2):
            for r in range(0, FULL, RC):
                rr = pl.ds(r, RC)
                xr, xi = natural(fld, mode, r)
                put(lh, 0, mode, rr, pl.ds(0, HALF), xr[:, :HALF])
                put(lh, 0, mode, rr, pl.ds(HALF, HALF), xi[:, :HALF])
                put(lh, 1, mode, rr, pl.ds(0, HALF), xr[:, HALF:])
                put(lh, 1, mode, rr, pl.ds(HALF, HALF), xi[:, HALF:])
        right(lh, mo, kh, kl, GS, GT)

        def wave_back(mode, rr):
            p, q = mo[0, mode, rr], mo[1, mode, rr]
            y0, y1 = p + q, p - q
            qr = jnp.concatenate([y0[:, :HALF], y1[:, :HALF]], axis=1)
            qi = jnp.concatenate([y0[:, HALF:], y1[:, HALF:]], axis=1)
            return qr, qi

        @pl.when(d == 0)
        def _():
            for mode in range(2):
                for r in range(0, FULL, RC):
                    rr = pl.ds(r, RC)
                    qr, qi = wave_back(mode, rr)
                    wr, wi = win[0, rr], win[1, rr]
                    halves_to_lh(lh, mode, r, wr * qr + wi * qi, wr * qi - wi * qr)
            right(lh, mo, kh, kl, CS, CT)
            prop_middle(mo, rh)
            left(rh, fld, kh, kl, MS, MT)
            for r in range(0, FULL, RC):
                rr = pl.ds(r, RC)
                vr = vi = None
                for mode in range(2):
                    qr, qi = natural(fld, mode, r)
                    pr, pi = probes[mode][0, rr], probes[mode][1, rr]
                    ar, ai = pr * qr + pi * qi, pr * qi - pi * qr
                    vr, vi = (ar, ai) if vr is None else (vr + ar, vi + ai)
                win[0, rr] = vr
                win[1, rr] = vi

        @pl.when(d != 0)
        def _():
            for r in range(0, FULL, RC):
                rr = pl.ds(r, RC)
                vr = vi = None
                for mode in range(2):
                    qr, qi = wave_back(mode, rr)
                    pr, pi = psi[mode, 0, rr], psi[mode, 1, rr]
                    ar, ai = pr * qr + pi * qi, pr * qi - pi * qr
                    vr, vi = (ar, ai) if vr is None else (vr + ar, vi + ai)
                win[0, rr] = vr
                win[1, rr] = vi

        top, q, shift = place(info, pos)
        lane = lax.broadcasted_iota(jnp.int32, (RC, HALF), 1)
        fwd = jnp.where(shift == HALF, 0, shift)
        later = lane >= shift
        zero = jnp.zeros((RC, HALF), F32)
        for c in range(2):
            for r in range(0, FULL, RC):
                rr = pl.ds(r, RC)
                r0 = pltpu.roll(win[c, rr, pl.ds(0, HALF)], fwd, axis=1)
                r1 = pltpu.roll(win[c, rr, pl.ds(HALF, HALF)], fwd, axis=1)
                vals = (jnp.where(later, r0, zero), jnp.where(later, r1, r0), jnp.where(later, zero, r1))
                for b in range(3):
                    acc[q + b, c, pl.ds(top + r, RC), :] = acc[q + b, c, pl.ds(top + r, RC), :] + vals[b]
        return carry

    lax.fori_loop(0, 2, position, 0)
    for blk, out in ((0, g_on), (1, g_o), (2, g_i), (3, g_in)):
        out[...] = acc[blk + odd * (3 - 2 * blk)]


def merge(a, b, ra, rb, out, buf, sem):
    odd = lax.axis_index("tile") % 2
    copies = []
    for c in range(2):
        buf[c, :, pl.ds(pl.multiple_of(odd * HALF, HALF), HALF)] = a[c] + ra[c]
        buf[c, :, pl.ds(pl.multiple_of((1 - odd) * HALF, HALF), HALF)] = b[c] + rb[c]
        copies.append(pltpu.make_async_copy(buf.at[c], out.at[0, c], sem.at[c]))
        copies[-1].start()
    for copy in copies:
        copy.wait()


def step(probe, object_slices, positions, measured):
    tiles = lax.axis_size("tile")
    cross = [(0, 3), (3, 0), (1, 2), (2, 1)]
    pair = [(i, i ^ 1) for i in range(tiles)]
    side = [(i, i + 1) for i in range(1, tiles - 1, 2)]
    side = side + [(j, i) for i, j in side]
    smem = pl.BlockSpec(memory_space=pltpu.SMEM)
    vmem = pl.BlockSpec(memory_space=pltpu.VMEM)
    anyw = pl.BlockSpec(memory_space=pltpu.HBM)
    block = pltpu.VMEM((2, ROWS, HALF), F32)
    own_o, own_i = pl.pallas_call(
        halve,
        out_shape=(block, block),
        in_specs=[anyw],
        out_specs=(vmem, vmem),
        scratch_shapes=[pltpu.SemaphoreType.DMA((2,))],
        name="halve",
        compiler_params=pltpu.CompilerParams(vmem_limit_bytes=2**20),
    )(in_hbm(object_slices))
    oth_o = lax.ppermute(own_o, ("depth", "mode"), cross)
    oth_i = lax.ppermute(own_i, ("depth", "mode"), cross)
    own_on = lax.ppermute(own_o, "tile", side)
    own_in = lax.ppermute(own_i, "tile", pair)
    prb = lax.ppermute(probe, "mode", [(0, 1), (1, 0)])
    oth_on = lax.ppermute(oth_o, "tile", side)
    oth_in = lax.ppermute(oth_i, "tile", pair)
    info = positions
    high, low, sort = (jnp.asarray(x) for x in tables())
    p1 = in_vmem(prb[0])
    wown, psi, mp, kh, kl, p0 = pl.pallas_call(
        early,
        out_shape=(pltpu.VMEM((2, 2, FULL, FULL), F32), pltpu.VMEM((2, 2, 2, FULL, FULL), F32),
                   pltpu.VMEM((2, 2, HALF, FULL), F32), pltpu.VMEM(high.shape, BF16),
                   pltpu.VMEM(low.shape, BF16), pltpu.VMEM((2, FULL, FULL), F32)),
        in_specs=[smem] + [vmem] * 4 + [anyw, vmem] + [anyw] * 4,
        out_specs=(vmem,) * 6,
        scratch_shapes=[
            pltpu.VMEM((4, 2, ROWS, HALF), F32),
            pltpu.VMEM((2, 2, 2, FULL, FULL), BF16),
            pltpu.VMEM((2, 2, 2, FULL, FULL), BF16),
            pltpu.VMEM((2, 2, FULL, FULL), F32),
            pltpu.VMEM((2, 2, FULL, FULL), F32),
            pltpu.VMEM((2, FULL, HALF), F32),
            pltpu.VMEM((2, FULL, FULL), F32),
            pltpu.VMEM((FULL, FULL), BF16),
            pltpu.SemaphoreType.DMA((5,)),
        ],
        name="early",
        compiler_params=pltpu.CompilerParams(vmem_limit_bytes=LIMIT),
    )(info, *map(in_vmem, (own_o, own_i, own_on, own_in)), in_hbm(probe), p1, *map(in_hbm, (measured, high, low, sort)))
    g_o, g_i, g_on, g_in = pl.pallas_call(
        grad,
        out_shape=(block,) * 4,
        in_specs=[smem] + [vmem] * 11,
        out_specs=(vmem,) * 4,
        scratch_shapes=[
            pltpu.VMEM((4, 2, ROWS, HALF), F32),
            pltpu.VMEM((4, 2, ROWS, HALF), F32),
            pltpu.VMEM((2, FULL, FULL), F32),
            pltpu.VMEM((2, 2, FULL, FULL), F32),
            pltpu.VMEM((2, 2, 2, FULL, FULL), BF16),
            pltpu.VMEM((2, 2, 2, FULL, FULL), BF16),
            pltpu.VMEM((2, 2, FULL, FULL), F32),
            pltpu.VMEM((2, 2, FULL, FULL), F32),
        ],
        name="grad",
        compiler_params=pltpu.CompilerParams(vmem_limit_bytes=LIMIT),
    )(info, *map(in_vmem, (oth_o, oth_i, oth_on, oth_in, wown, psi, mp, p0)), p1, in_vmem(kh), in_vmem(kl))
    r_o = lax.ppermute(g_on, "tile", side)
    r_i = lax.ppermute(g_in, "tile", pair)
    return pl.pallas_call(
        merge,
        out_shape=jax.ShapeDtypeStruct((1, 2, ROWS, FULL), F32),
        in_specs=[vmem] * 4,
        out_specs=anyw,
        scratch_shapes=[pltpu.VMEM((2, ROWS, FULL), F32), pltpu.SemaphoreType.DMA((2,))],
        name="merge",
        compiler_params=pltpu.CompilerParams(vmem_limit_bytes=LIMIT),
    )(*map(in_vmem, (g_o, g_i, r_o, r_i)))


def in_hbm(x):
    return pltpu.with_memory_space_constraint(x, pltpu.HBM)


def in_vmem(x):
    return pltpu.with_memory_space_constraint(x, pltpu.VMEM)


def solution(mesh):
    placed = (
        P("mode", None, None, None),
        P("depth", None, None, "tile"),
        P("tile", None),
        P("tile", None, None),
    )
    return jax.shard_map(
        step, mesh=mesh, in_specs=placed, out_specs=P("depth", None, None, "tile"), check_vma=False
    )
```

```python
import numpy as np

import jax
import jax.numpy as jnp
from jax import lax
from jax.experimental import pallas as pl
from jax.experimental.pallas import tpu as pltpu
from jax.sharding import PartitionSpec as P


HALF = 128
FULL = 256
ROWS = 384
F32 = jnp.float32
BF16 = jnp.bfloat16
FS, FT, GS, GT, MS, MT, CS, CT = range(8)


def tables():
    n = np.arange(HALF)
    unit = lambda k: np.exp(-2j * np.pi * (k % FULL) / FULL) / 16.0
    even = unit(2 * n[:, None] * n[None, :])
    odd = unit(n[:, None] * (2 * n[None, :] + 1))
    j = np.arange(FULL)
    dft = unit(j[:, None] * j[None, :])
    f = np.where(j < HALF, j, j - FULL)
    h = np.exp(-2j * np.pi * (3 * f * f % 1024) / 1024)
    prop = dft.conj() @ (h[:, None] * dft)
    near, far = prop[:HALF, :HALF], prop[:HALF, HALF:]
    ms, mt = (near + far) / 2, (near - far) / 2
    pairs = lambda c: np.block([[c.real, c.imag], [-c.imag, c.real]])
    mats = [even, odd, even.conj(), odd.conj().T, ms, mt, ms.conj(), mt.conj()]
    whole = np.stack([pairs(c) for c in mats]).astype(np.float32)
    high = whole.astype(jnp.bfloat16)
    low = (whole - high.astype(np.float32)).astype(jnp.bfloat16)
    src = np.concatenate([np.arange(0, FULL, 2), np.arange(1, FULL, 2)])
    sort = np.zeros((FULL, FULL), np.float32)
    sort[src, np.arange(FULL)] = 1.0
    return high, low, sort.astype(jnp.bfloat16)


def split(x):
    high = x.astype(BF16)
    return high, (x - high.astype(F32)).astype(BF16)


def dot(a, b):
    return jnp.dot(a, b, preferred_element_type=F32)


RC = 32
LIMIT = 20 * 2**20


def put(ref, k, mode, rows, cols, value):
    high, low = split(value)
    ref[0, k, mode, rows, cols] = high
    ref[1, k, mode, rows, cols] = low


def right(lh, mo, kh, kl, ks, kt):
    for mode in range(2):
        for k, kk in ((0, ks), (1, kt)):
            for r in range(0, FULL, HALF):
                rr = pl.ds(r, HALF)
                xh, xl = lh[0, k, mode, rr], lh[1, k, mode, rr]
                mo[k, mode, rr] = dot(xh, kh[kk]) + (dot(xh, kl[kk]) + dot(xl, kh[kk]))


def left(rh, dst, kh, kl, ks, kt):
    for mode in range(2):
        for k, kk in ((0, ks), (1, kt)):
            for r in range(0, FULL, HALF):
                rr = pl.ds(r, HALF)
                ch, cl = kh[kk, rr], kl[kk, rr]
                xh, xl = rh[0, k, mode], rh[1, k, mode]
                dst[k, mode, rr] = dot(ch, xh) + (dot(cl, xh) + dot(ch, xl))


def halves_to_lh(lh, mode, r, ur, ui):
    rows = pl.ds(r, RC)
    a, b = ur[:, :HALF], ur[:, HALF:]
    c, e = ui[:, :HALF], ui[:, HALF:]
    put(lh, 0, mode, rows, pl.ds(0, HALF), a + b)
    put(lh, 1, mode, rows, pl.ds(0, HALF), a - b)
    put(lh, 0, mode, rows, pl.ds(HALF, HALF), c + e)
    put(lh, 1, mode, rows, pl.ds(HALF, HALF), c - e)


def prop_middle(mo, rh):
    for mode in range(2):
        for r in range(0, HALF, RC):
            top, bot = pl.ds(r, RC), pl.ds(HALF + r, RC)
            pt, qt = mo[0, mode, top], mo[1, mode, top]
            pb, qb = mo[0, mode, bot], mo[1, mode, bot]
            for sign, k in ((1, 0), (-1, 1)):
                p = pt + pb if sign > 0 else pt - pb
                q = qt + qb if sign > 0 else qt - qb
                y0, y1 = p + q, p - q
                put(rh, k, mode, top, pl.ds(0, HALF), y0[:, :HALF])
                put(rh, k, mode, top, pl.ds(HALF, HALF), y1[:, :HALF])
                put(rh, k, mode, bot, pl.ds(0, HALF), y0[:, HALF:])
                put(rh, k, mode, bot, pl.ds(HALF, HALF), y1[:, HALF:])


def natural(src, mode, r):
    base = r % HALF
    top, bot = pl.ds(base, RC), pl.ds(HALF + base, RC)
    if r < HALF:
        return src[0, mode, top] + src[1, mode, top], src[0, mode, bot] + src[1, mode, bot]
    return src[0, mode, top] - src[1, mode, top], src[0, mode, bot] - src[1, mode, bot]


def place(info, pos):
    top = info[pos, 0]
    col = info[pos, 1]
    q = jnp.where(col >= HALF, 1, 0)
    return top, q, col - q * HALF


def gather(odd, parts, ext):
    outer, inner, far_outer, far_inner = parts
    for blk, src in ((0, far_outer), (1, outer), (2, inner), (3, far_inner)):
        ext[blk + odd * (3 - 2 * blk)] = src[...]


def cut(info, pos, ext, store):
    top, q, shift = place(info, pos)
    lane = lax.broadcasted_iota(jnp.int32, (RC, HALF), 1)
    back = jnp.where(shift == 0, 0, HALF - shift)
    keep = lane < HALF - shift
    for c in range(2):
        for r in range(0, FULL, RC):
            rot = [pltpu.roll(ext[q + b, c, pl.ds(top + r, RC), :], back, axis=1) for b in range(3)]
            store(c, pl.ds(r, RC), pl.ds(0, HALF), jnp.where(keep, rot[0], rot[1]))
            store(c, pl.ds(r, RC), pl.ds(HALF, HALF), jnp.where(keep, rot[1], rot[2]))


def halve(whole, outer, inner, sem):
    odd = lax.axis_index("tile") % 2
    copies = []
    for k, (side, half) in enumerate(((odd, outer), (1 - odd, inner))):
        lanes = pl.ds(pl.multiple_of(side * HALF, HALF), HALF)
        copies.append(pltpu.make_async_copy(whole.at[0, :, :, lanes], half, sem.at[k]))
        copies[-1].start()
    for copy in copies:
        copy.wait()


def prepare(where, prb_hbm, meas_hbm, kh_hbm, kl_hbm, sort_hbm, info, mp, kh, kl, prb0, cols, meas, sort, sem):
    moves = [(meas_hbm, meas), (sort_hbm, sort), (kh_hbm, kh), (kl_hbm, kl), (prb_hbm.at[0], prb0)]
    copies = [pltpu.make_async_copy(src, dst, sem.at[k]) for k, (src, dst) in enumerate(moves)]
    for copy in copies:
        copy.start()
    for pos in range(2):
        for k in range(2):
            info[pos, k] = where[pos, k]
    for copy in copies[:2]:
        copy.wait()
    for pos in range(2):
        for c in range(2):
            cols[c] = meas[pos, :, pl.ds(c * HALF, HALF)]
        for par in range(2):
            m = jnp.concatenate([cols[c, pl.ds(par, HALF, stride=2), :] for c in range(2)], axis=1)
            m1 = m.astype(BF16)
            rest = m - m1.astype(F32)
            m2 = rest.astype(BF16)
            m3 = (rest - m2.astype(F32)).astype(BF16)
            mp[pos, par] = dot(m1, sort[...]) + (dot(m2, sort[...]) + dot(m3, sort[...]))
    for copy in copies[2:]:
        copy.wait()


def early(info, own_o, own_i, own_on, own_in, prb0, prb1, kh, kl, wown, psi, ext, lh, rh, mo, fld):
    d = lax.axis_index("depth")
    gather(lax.axis_index("tile") % 2, (own_o, own_i, own_on, own_in), ext)
    probes = (prb0, prb1)

    def position(pos, carry):
        def store(c, rows, at, value):
            wown[pos, c, rows, at] = value

        cut(info, pos, ext, store)

        @pl.when(d == 0)
        def _():
            for mode in range(2):
                for r in range(0, FULL, RC):
                    rr = pl.ds(r, RC)
                    pr, pi = probes[mode][0, rr], probes[mode][1, rr]
                    wr, wi = wown[pos, 0, rr], wown[pos, 1, rr]
                    halves_to_lh(lh, mode, r, pr * wr - pi * wi, pr * wi + pi * wr)
            right(lh, mo, kh, kl, MS, MT)
            prop_middle(mo, rh)
            left(rh, fld, kh, kl, CS, CT)
            for mode in range(2):
                for r in range(0, FULL, RC):
                    pr, pi = natural(fld, mode, r)
                    psi[pos, mode, 0, pl.ds(r, RC)] = pr
                    psi[pos, mode, 1, pl.ds(r, RC)] = pi

        return carry

    lax.fori_loop(0, 2, position, 0)


def grad(info, oth_o, oth_i, oth_on, oth_in, wown, psi0, mp, prb0, prb1, kh, kl, g_o, g_i, g_on, g_in,
         ext, acc, win, psi, lh, rh, mo, fld):
    d = lax.axis_index("depth")
    odd = lax.axis_index("tile") % 2
    gather(odd, (oth_o, oth_i, oth_on, oth_in), ext)
    acc[...] = jnp.zeros(acc.shape, F32)
    probes = (prb0, prb1)

    def position(pos, carry):
        def store(c, rows, at, value):
            win[c, rows, at] = value

        cut(info, pos, ext, store)

        @pl.when(d == 0)
        def _():
            for mode in range(2):
                for r in range(0, FULL, RC):
                    rr = pl.ds(r, RC)
                    pr, pi = psi0[pos, mode, 0, rr], psi0[pos, mode, 1, rr]
                    wr, wi = win[0, rr], win[1, rr]
                    halves_to_lh(lh, mode, r, pr * wr - pi * wi, pr * wi + pi * wr)

        @pl.when(d != 0)
        def _():
            for mode in range(2):
                for r in range(0, FULL, RC):
                    rr = pl.ds(r, RC)
                    pr, pi = probes[mode][0, rr], probes[mode][1, rr]
                    wr, wi = win[0, rr], win[1, rr]
                    halves_to_lh(lh, mode, r, pr * wr - pi * wi, pr * wi + pi * wr)
            right(lh, mo, kh, kl, MS, MT)
            prop_middle(mo, rh)
            left(rh, fld, kh, kl, CS, CT)
            for mode in range(2):
                for r in range(0, FULL, RC):
                    rr = pl.ds(r, RC)
                    pr, pi = natural(fld, mode, r)
                    psi[mode, 0, rr] = pr
                    psi[mode, 1, rr] = pi
                    wr, wi = wown[pos, 0, rr], wown[pos, 1, rr]
                    halves_to_lh(lh, mode, r, pr * wr - pi * wi, pr * wi + pi * wr)

        right(lh, mo, kh, kl, FS, FT)
        for mode in range(2):
            for r in range(0, HALF, RC):
                tp, bt = pl.ds(r, RC), pl.ds(HALF + r, RC)
                for c in range(2):
                    et, eb = mo[c, mode, tp], mo[c, mode, bt]
                    s, t = et + eb, et - eb
                    at = pl.ds(c * HALF, HALF)
                    put(rh, 0, mode, tp, at, s[:, :HALF])
                    put(rh, 0, mode, bt, at, s[:, HALF:])
                    put(rh, 1, mode, tp, at, t[:, :HALF])
                    put(rh, 1, mode, bt, at, t[:, HALF:])
        left(rh, fld, kh, kl, GS, GT)
        for par in range(2):
            for r in range(0, HALF, RC):
                tp, bt = pl.ds(r, RC), pl.ds(HALF + r, RC)
                fr = [fld[par, mode, tp] for mode in range(2)]
                fi = [fld[par, mode, bt] for mode in range(2)]
                resid = (fr[0] * fr[0] + fi[0] * fi[0]) + (fr[1] * fr[1] + fi[1] * fi[1]) - mp[pos, par, tp]
                for mode in range(2):
                    put(rh, par, mode, tp, slice(None), resid * fr[mode])
                    put(rh, par, mode, bt, slice(None), resid * fi[mode])
        left(rh, fld, kh, kl, FS, FT)
        for mode in range(2):
            for r in range(0, FULL, RC):
                rr = pl.ds(r, RC)
                xr, xi = natural(fld, mode, r)
                put(lh, 0, mode, rr, pl.ds(0, HALF), xr[:, :HALF])
                put(lh, 0, mode, rr, pl.ds(HALF, HALF), xi[:, :HALF])
                put(lh, 1, mode, rr, pl.ds(0, HALF), xr[:, HALF:])
                put(lh, 1, mode, rr, pl.ds(HALF, HALF), xi[:, HALF:])
        right(lh, mo, kh, kl, GS, GT)

        def wave_back(mode, rr):
            p, q = mo[0, mode, rr], mo[1, mode, rr]
            y0, y1 = p + q, p - q
            qr = jnp.concatenate([y0[:, :HALF], y1[:, :HALF]], axis=1)
            qi = jnp.concatenate([y0[:, HALF:], y1[:, HALF:]], axis=1)
            return qr, qi

        @pl.when(d == 0)
        def _():
            for mode in range(2):
                for r in range(0, FULL, RC):
                    rr = pl.ds(r, RC)
                    qr, qi = wave_back(mode, rr)
                    wr, wi = win[0, rr], win[1, rr]
                    halves_to_lh(lh, mode, r, wr * qr + wi * qi, wr * qi - wi * qr)
            right(lh, mo, kh, kl, CS, CT)
            prop_middle(mo, rh)
            left(rh, fld, kh, kl, MS, MT)
            for r in range(0, FULL, RC):
                rr = pl.ds(r, RC)
                vr = vi = None
                for mode in range(2):
                    qr, qi = natural(fld, mode, r)
                    pr, pi = probes[mode][0, rr], probes[mode][1, rr]
                    ar, ai = pr * qr + pi * qi, pr * qi - pi * qr
                    vr, vi = (ar, ai) if vr is None else (vr + ar, vi + ai)
                win[0, rr] = vr
                win[1, rr] = vi

        @pl.when(d != 0)
        def _():
            for r in range(0, FULL, RC):
                rr = pl.ds(r, RC)
                vr = vi = None
                for mode in range(2):
                    qr, qi = wave_back(mode, rr)
                    pr, pi = psi[mode, 0, rr], psi[mode, 1, rr]
                    ar, ai = pr * qr + pi * qi, pr * qi - pi * qr
                    vr, vi = (ar, ai) if vr is None else (vr + ar, vi + ai)
                win[0, rr] = vr
                win[1, rr] = vi

        top, q, shift = place(info, pos)
        lane = lax.broadcasted_iota(jnp.int32, (RC, HALF), 1)
        fwd = jnp.where(shift == HALF, 0, shift)
        later = lane >= shift
        zero = jnp.zeros((RC, HALF), F32)
        for c in range(2):
            for r in range(0, FULL, RC):
                rr = pl.ds(r, RC)
                r0 = pltpu.roll(win[c, rr, pl.ds(0, HALF)], fwd, axis=1)
                r1 = pltpu.roll(win[c, rr, pl.ds(HALF, HALF)], fwd, axis=1)
                vals = (jnp.where(later, r0, zero), jnp.where(later, r1, r0), jnp.where(later, zero, r1))
                for b in range(3):
                    acc[q + b, c, pl.ds(top + r, RC), :] = acc[q + b, c, pl.ds(top + r, RC), :] + vals[b]
        return carry

    lax.fori_loop(0, 2, position, 0)
    for blk, out in ((0, g_on), (1, g_o), (2, g_i), (3, g_in)):
        out[...] = acc[blk + odd * (3 - 2 * blk)]


def merge(a, b, ra, rb, out, buf, sem):
    odd = lax.axis_index("tile") % 2
    copies = []
    for c in range(2):
        buf[c, :, pl.ds(pl.multiple_of(odd * HALF, HALF), HALF)] = a[c] + ra[odd, c]
        buf[c, :, pl.ds(pl.multiple_of((1 - odd) * HALF, HALF), HALF)] = b[c] + rb[c]
        copies.append(pltpu.make_async_copy(buf.at[c], out.at[0, c], sem.at[c]))
        copies[-1].start()
    for copy in copies:
        copy.wait()


def step(probe, object_slices, positions, measured):
    tiles = lax.axis_size("tile")
    cross = [(0, 3), (3, 0), (1, 2), (2, 1)]
    pair = [(i, i ^ 1) for i in range(tiles)]
    side = [(i, i + 1) for i in range(1, tiles - 1, 2)]
    side = side + [(j, i) for i, j in side]
    smem = pl.BlockSpec(memory_space=pltpu.SMEM)
    vmem = pl.BlockSpec(memory_space=pltpu.VMEM)
    anyw = pl.BlockSpec(memory_space=pltpu.HBM)
    block = pltpu.VMEM((2, ROWS, HALF), F32)
    own_o, own_i = pl.pallas_call(
        halve,
        out_shape=(block, block),
        in_specs=[anyw],
        out_specs=(vmem, vmem),
        scratch_shapes=[pltpu.SemaphoreType.DMA((2,))],
        name="halve",
        compiler_params=pltpu.CompilerParams(vmem_limit_bytes=2**20),
    )(in_hbm(object_slices))
    oth_o = lax.ppermute(own_o, ("depth", "mode"), cross)
    oth_i = lax.ppermute(own_i, ("depth", "mode"), cross)
    own_on = lax.ppermute(own_o, "tile", side)
    own_in = lax.ppermute(own_i, "tile", pair)
    prb = lax.ppermute(probe, "mode", [(0, 1), (1, 0)])
    oth_on = lax.ppermute(oth_o, "tile", side)
    oth_in = lax.ppermute(oth_i, "tile", pair)
    high, low, sort = (jnp.asarray(x) for x in tables())
    limit = pltpu.CompilerParams(vmem_limit_bytes=LIMIT)
    pair_of = pltpu.VMEM((2, 2, FULL, FULL), F32)
    info, mp, kh, kl, p0 = pl.pallas_call(
        prepare,
        out_shape=(pltpu.SMEM((2, 2), jnp.int32), pltpu.VMEM((2, 2, HALF, FULL), F32), pltpu.VMEM(high.shape, BF16),
                   pltpu.VMEM(low.shape, BF16), pltpu.VMEM((2, FULL, FULL), F32)),
        in_specs=[smem] + [anyw] * 5,
        out_specs=(smem,) + (vmem,) * 4,
        scratch_shapes=[
            pltpu.VMEM((2, FULL, HALF), F32),
            pltpu.VMEM((2, FULL, FULL), F32),
            pltpu.VMEM((FULL, FULL), BF16),
            pltpu.SemaphoreType.DMA((5,)),
        ],
        name="prepare",
        compiler_params=limit,
    )(positions, *map(in_hbm, (probe, measured, high, low, sort)))
    info = pltpu.with_memory_space_constraint(info, pltpu.SMEM)
    p0, p1, kh, kl, mp = map(in_vmem, (p0, prb[0], kh, kl, mp))
    fields = [pltpu.VMEM((2, 2, 2, FULL, FULL), BF16)] * 2 + [pair_of] * 2
    wown, psi = pl.pallas_call(
        early,
        out_shape=(pair_of, pltpu.VMEM((2, 2, 2, FULL, FULL), F32)),
        in_specs=[smem] + [vmem] * 8,
        out_specs=(vmem,) * 2,
        scratch_shapes=[pltpu.VMEM((4, 2, ROWS, HALF), F32)] + fields,
        name="early",
        compiler_params=limit,
    )(info, *map(in_vmem, (own_o, own_i, own_on, own_in)), p0, p1, kh, kl)
    g_o, g_i, g_on, g_in = pl.pallas_call(
        grad,
        out_shape=(block,) * 4,
        in_specs=[smem] + [vmem] * 11,
        out_specs=(vmem,) * 4,
        scratch_shapes=[
            pltpu.VMEM((4, 2, ROWS, HALF), F32),
            pltpu.VMEM((4, 2, ROWS, HALF), F32),
            pltpu.VMEM((2, FULL, FULL), F32),
            pair_of,
        ] + fields,
        name="grad",
        compiler_params=limit,
    )(info, *map(in_vmem, (oth_o, oth_i, oth_on, oth_in, wown, psi)), mp, p0, p1, kh, kl)
    groups = [[m * tiles + i, m * tiles + i + 1] for m in range(2) for i in range(1, tiles - 1, 2)]
    groups = groups + [[i, tiles + i] for i in (0, tiles - 1)]
    r_i = lax.ppermute(g_in, "tile", pair)
    r_o = lax.all_gather(g_on, ("mode", "tile"), axis_index_groups=groups)
    return pl.pallas_call(
        merge,
        out_shape=jax.ShapeDtypeStruct((1, 2, ROWS, FULL), F32),
        in_specs=[vmem] * 4,
        out_specs=anyw,
        scratch_shapes=[pltpu.VMEM((2, ROWS, FULL), F32), pltpu.SemaphoreType.DMA((2,))],
        name="merge",
        compiler_params=pltpu.CompilerParams(vmem_limit_bytes=LIMIT),
    )(*map(in_vmem, (g_o, g_i, r_o, r_i)))


def in_hbm(x):
    return pltpu.with_memory_space_constraint(x, pltpu.HBM)


def in_vmem(x):
    return pltpu.with_memory_space_constraint(x, pltpu.VMEM)


def solution(mesh):
    placed = (
        P("mode", None, None, None),
        P("depth", None, None, "tile"),
        P("tile", None),
        P("tile", None, None),
    )
    return jax.shard_map(step, mesh=mesh, in_specs=placed, out_specs=P("depth", None, None, "tile"), check_vma=False)
```

```python
import numpy as np

import jax
import jax.numpy as jnp
from jax import lax
from jax.experimental import pallas as pl
from jax.experimental.pallas import tpu as pltpu
from jax.sharding import PartitionSpec as P


HALF = 128
FULL = 256
ROWS = 384
F32 = jnp.float32
BF16 = jnp.bfloat16
FS, FT, GS, GT, MS, MT, CS, CT = range(8)


def tables():
    n = np.arange(HALF)
    unit = lambda k: np.exp(-2j * np.pi * (k % FULL) / FULL) / 16.0
    even = unit(2 * n[:, None] * n[None, :])
    odd = unit(n[:, None] * (2 * n[None, :] + 1))
    j = np.arange(FULL)
    dft = unit(j[:, None] * j[None, :])
    f = np.where(j < HALF, j, j - FULL)
    h = np.exp(-2j * np.pi * (3 * f * f % 1024) / 1024)
    prop = dft.conj() @ (h[:, None] * dft)
    near, far = prop[:HALF, :HALF], prop[:HALF, HALF:]
    ms, mt = (near + far) / 2, (near - far) / 2
    pairs = lambda c: np.block([[c.real, c.imag], [-c.imag, c.real]])
    mats = [even, odd, even.conj(), odd.conj().T, ms, mt, ms.conj(), mt.conj()]
    whole = np.stack([pairs(c) for c in mats]).astype(np.float32)
    high = whole.astype(jnp.bfloat16)
    low = (whole - high.astype(np.float32)).astype(jnp.bfloat16)
    src = np.concatenate([np.arange(0, FULL, 2), np.arange(1, FULL, 2)])
    sort = np.zeros((FULL, FULL), np.float32)
    sort[src, np.arange(FULL)] = 1.0
    return high, low, sort.astype(jnp.bfloat16)


def split(x):
    high = x.astype(BF16)
    return high, (x - high.astype(F32)).astype(BF16)


def dot(a, b):
    return jnp.dot(a, b, preferred_element_type=F32)


RC = 64
LIMIT = 20 * 2**20


def put(ref, k, mode, rows, cols, value):
    high, low = split(value)
    ref[0, k, mode, rows, cols] = high
    ref[1, k, mode, rows, cols] = low


def right(lh, mo, kh, kl, ks, kt):
    for mode in range(2):
        for k, kk in ((0, ks), (1, kt)):
            for r in range(0, FULL, HALF):
                rr = pl.ds(r, HALF)
                xh, xl = lh[0, k, mode, rr], lh[1, k, mode, rr]
                mo[k, mode, rr] = dot(xh, kh[kk]) + (dot(xh, kl[kk]) + dot(xl, kh[kk]))


def left(rh, dst, kh, kl, ks, kt):
    for mode in range(2):
        for k, kk in ((0, ks), (1, kt)):
            for r in range(0, FULL, HALF):
                rr = pl.ds(r, HALF)
                ch, cl = kh[kk, rr], kl[kk, rr]
                xh, xl = rh[0, k, mode], rh[1, k, mode]
                dst[k, mode, rr] = dot(ch, xh) + (dot(cl, xh) + dot(ch, xl))


def halves_to_lh(lh, mode, r, ur, ui):
    rows = pl.ds(r, RC)
    a, b = ur[:, :HALF], ur[:, HALF:]
    c, e = ui[:, :HALF], ui[:, HALF:]
    put(lh, 0, mode, rows, pl.ds(0, HALF), a + b)
    put(lh, 1, mode, rows, pl.ds(0, HALF), a - b)
    put(lh, 0, mode, rows, pl.ds(HALF, HALF), c + e)
    put(lh, 1, mode, rows, pl.ds(HALF, HALF), c - e)


def prop_middle(mo, rh):
    for mode in range(2):
        for r in range(0, HALF, RC):
            top, bot = pl.ds(r, RC), pl.ds(HALF + r, RC)
            pt, qt = mo[0, mode, top], mo[1, mode, top]
            pb, qb = mo[0, mode, bot], mo[1, mode, bot]
            for sign, k in ((1, 0), (-1, 1)):
                p = pt + pb if sign > 0 else pt - pb
                q = qt + qb if sign > 0 else qt - qb
                y0, y1 = p + q, p - q
                put(rh, k, mode, top, pl.ds(0, HALF), y0[:, :HALF])
                put(rh, k, mode, top, pl.ds(HALF, HALF), y1[:, :HALF])
                put(rh, k, mode, bot, pl.ds(0, HALF), y0[:, HALF:])
                put(rh, k, mode, bot, pl.ds(HALF, HALF), y1[:, HALF:])


def natural(src, mode, r):
    base = r % HALF
    top, bot = pl.ds(base, RC), pl.ds(HALF + base, RC)
    if r < HALF:
        return src[0, mode, top] + src[1, mode, top], src[0, mode, bot] + src[1, mode, bot]
    return src[0, mode, top] - src[1, mode, top], src[0, mode, bot] - src[1, mode, bot]


def place(info, pos):
    top = info[pos, 0]
    col = info[pos, 1]
    q = jnp.where(col >= HALF, 1, 0)
    return top, q, col - q * HALF


def gather(odd, parts, ext):
    outer, inner, far_outer, far_inner = parts
    for blk, src in ((0, far_outer), (1, outer), (2, inner), (3, far_inner)):
        ext[blk + odd * (3 - 2 * blk)] = src[...]


def cut(info, pos, ext, store):
    top, q, shift = place(info, pos)
    lane = lax.broadcasted_iota(jnp.int32, (RC, HALF), 1)
    back = jnp.where(shift == 0, 0, HALF - shift)
    keep = lane < HALF - shift
    for c in range(2):
        for r in range(0, FULL, RC):
            rot = [pltpu.roll(ext[q + b, c, pl.ds(top + r, RC), :], back, axis=1) for b in range(3)]
            store(c, pl.ds(r, RC), pl.ds(0, HALF), jnp.where(keep, rot[0], rot[1]))
            store(c, pl.ds(r, RC), pl.ds(HALF, HALF), jnp.where(keep, rot[1], rot[2]))


def halve(whole, outer, inner, sem):
    odd = lax.axis_index("tile") % 2
    copies = []
    for k, (side, half) in enumerate(((odd, outer), (1 - odd, inner))):
        lanes = pl.ds(pl.multiple_of(side * HALF, HALF), HALF)
        copies.append(pltpu.make_async_copy(whole.at[0, :, :, lanes], half, sem.at[k]))
        copies[-1].start()
    for copy in copies:
        copy.wait()


def prepare(where, prb_hbm, meas_hbm, kh_hbm, kl_hbm, sort_hbm, info, mp, kh, kl, prb0, cols, meas, sort, sem):
    moves = [(meas_hbm, meas), (sort_hbm, sort), (kh_hbm, kh), (kl_hbm, kl), (prb_hbm.at[0], prb0)]
    copies = [pltpu.make_async_copy(src, dst, sem.at[k]) for k, (src, dst) in enumerate(moves)]
    for copy in copies:
        copy.start()
    for pos in range(2):
        for k in range(2):
            info[pos, k] = where[pos, k]
    for copy in copies[:2]:
        copy.wait()
    for pos in range(2):
        for c in range(2):
            cols[c] = meas[pos, :, pl.ds(c * HALF, HALF)]
        for par in range(2):
            m = jnp.concatenate([cols[c, pl.ds(par, HALF, stride=2), :] for c in range(2)], axis=1)
            m1 = m.astype(BF16)
            rest = m - m1.astype(F32)
            m2 = rest.astype(BF16)
            m3 = (rest - m2.astype(F32)).astype(BF16)
            mp[pos, par] = dot(m1, sort[...]) + (dot(m2, sort[...]) + dot(m3, sort[...]))
    for copy in copies[2:]:
        copy.wait()


def early(info, own_o, own_i, own_on, own_in, prb0, prb1, kh, kl, wown, psi, ext, lh, rh, mo, fld):
    d = lax.axis_index("depth")
    gather(lax.axis_index("tile") % 2, (own_o, own_i, own_on, own_in), ext)
    probes = (prb0, prb1)

    def position(pos, carry):
        def store(c, rows, at, value):
            wown[pos, c, rows, at] = value

        cut(info, pos, ext, store)

        @pl.when(d == 0)
        def _():
            for mode in range(2):
                for r in range(0, FULL, RC):
                    rr = pl.ds(r, RC)
                    pr, pi = probes[mode][0, rr], probes[mode][1, rr]
                    wr, wi = wown[pos, 0, rr], wown[pos, 1, rr]
                    halves_to_lh(lh, mode, r, pr * wr - pi * wi, pr * wi + pi * wr)
            right(lh, mo, kh, kl, MS, MT)
            prop_middle(mo, rh)
            left(rh, fld, kh, kl, CS, CT)
            for mode in range(2):
                for r in range(0, FULL, RC):
                    pr, pi = natural(fld, mode, r)
                    psi[pos, mode, 0, pl.ds(r, RC)] = pr
                    psi[pos, mode, 1, pl.ds(r, RC)] = pi

        return carry

    lax.fori_loop(0, 2, position, 0)


def grad(info, oth_o, oth_i, oth_on, oth_in, wown, psi0, mp, prb0, prb1, kh, kl, g_o, g_i, g_on, g_in,
         ext, acc, win, psi, lh, rh, mo, fld):
    d = lax.axis_index("depth")
    odd = lax.axis_index("tile") % 2
    gather(odd, (oth_o, oth_i, oth_on, oth_in), ext)
    acc[...] = jnp.zeros(acc.shape, F32)
    probes = (prb0, prb1)

    def position(section0, pos, carry):
        def store(c, rows, at, value):
            win[c, rows, at] = value

        cut(info, pos, ext, store)

        if section0:
            for mode in range(2):
                for r in range(0, FULL, RC):
                    rr = pl.ds(r, RC)
                    pr, pi = psi0[pos, mode, 0, rr], psi0[pos, mode, 1, rr]
                    wr, wi = win[0, rr], win[1, rr]
                    halves_to_lh(lh, mode, r, pr * wr - pi * wi, pr * wi + pi * wr)

        if not section0:
            for mode in range(2):
                for r in range(0, FULL, RC):
                    rr = pl.ds(r, RC)
                    pr, pi = probes[mode][0, rr], probes[mode][1, rr]
                    wr, wi = win[0, rr], win[1, rr]
                    halves_to_lh(lh, mode, r, pr * wr - pi * wi, pr * wi + pi * wr)
            right(lh, mo, kh, kl, MS, MT)
            prop_middle(mo, rh)
            left(rh, fld, kh, kl, CS, CT)
            for mode in range(2):
                for r in range(0, FULL, RC):
                    rr = pl.ds(r, RC)
                    pr, pi = natural(fld, mode, r)
                    psi[mode, 0, rr] = pr
                    psi[mode, 1, rr] = pi
                    wr, wi = wown[pos, 0, rr], wown[pos, 1, rr]
                    halves_to_lh(lh, mode, r, pr * wr - pi * wi, pr * wi + pi * wr)

        right(lh, mo, kh, kl, FS, FT)
        for mode in range(2):
            for r in range(0, HALF, RC):
                tp, bt = pl.ds(r, RC), pl.ds(HALF + r, RC)
                for c in range(2):
                    et, eb = mo[c, mode, tp], mo[c, mode, bt]
                    s, t = et + eb, et - eb
                    at = pl.ds(c * HALF, HALF)
                    put(rh, 0, mode, tp, at, s[:, :HALF])
                    put(rh, 0, mode, bt, at, s[:, HALF:])
                    put(rh, 1, mode, tp, at, t[:, :HALF])
                    put(rh, 1, mode, bt, at, t[:, HALF:])
        left(rh, fld, kh, kl, GS, GT)
        for par in range(2):
            for r in range(0, HALF, RC):
                tp, bt = pl.ds(r, RC), pl.ds(HALF + r, RC)
                fr = [fld[par, mode, tp] for mode in range(2)]
                fi = [fld[par, mode, bt] for mode in range(2)]
                resid = (fr[0] * fr[0] + fi[0] * fi[0]) + (fr[1] * fr[1] + fi[1] * fi[1]) - mp[pos, par, tp]
                for mode in range(2):
                    put(rh, par, mode, tp, slice(None), resid * fr[mode])
                    put(rh, par, mode, bt, slice(None), resid * fi[mode])
        left(rh, fld, kh, kl, FS, FT)
        for mode in range(2):
            for r in range(0, FULL, RC):
                rr = pl.ds(r, RC)
                xr, xi = natural(fld, mode, r)
                put(lh, 0, mode, rr, pl.ds(0, HALF), xr[:, :HALF])
                put(lh, 0, mode, rr, pl.ds(HALF, HALF), xi[:, :HALF])
                put(lh, 1, mode, rr, pl.ds(0, HALF), xr[:, HALF:])
                put(lh, 1, mode, rr, pl.ds(HALF, HALF), xi[:, HALF:])
        right(lh, mo, kh, kl, GS, GT)

        def wave_back(mode, rr):
            p, q = mo[0, mode, rr], mo[1, mode, rr]
            y0, y1 = p + q, p - q
            qr = jnp.concatenate([y0[:, :HALF], y1[:, :HALF]], axis=1)
            qi = jnp.concatenate([y0[:, HALF:], y1[:, HALF:]], axis=1)
            return qr, qi

        if section0:
            for mode in range(2):
                for r in range(0, FULL, RC):
                    rr = pl.ds(r, RC)
                    qr, qi = wave_back(mode, rr)
                    wr, wi = win[0, rr], win[1, rr]
                    halves_to_lh(lh, mode, r, wr * qr + wi * qi, wr * qi - wi * qr)
            right(lh, mo, kh, kl, CS, CT)
            prop_middle(mo, rh)
            left(rh, fld, kh, kl, MS, MT)
            for r in range(0, FULL, RC):
                rr = pl.ds(r, RC)
                vr = vi = None
                for mode in range(2):
                    qr, qi = natural(fld, mode, r)
                    pr, pi = probes[mode][0, rr], probes[mode][1, rr]
                    ar, ai = pr * qr + pi * qi, pr * qi - pi * qr
                    vr, vi = (ar, ai) if vr is None else (vr + ar, vi + ai)
                win[0, rr] = vr
                win[1, rr] = vi

        if not section0:
            for r in range(0, FULL, RC):
                rr = pl.ds(r, RC)
                vr = vi = None
                for mode in range(2):
                    qr, qi = wave_back(mode, rr)
                    pr, pi = psi[mode, 0, rr], psi[mode, 1, rr]
                    ar, ai = pr * qr + pi * qi, pr * qi - pi * qr
                    vr, vi = (ar, ai) if vr is None else (vr + ar, vi + ai)
                win[0, rr] = vr
                win[1, rr] = vi

        top, q, shift = place(info, pos)
        lane = lax.broadcasted_iota(jnp.int32, (RC, HALF), 1)
        fwd = jnp.where(shift == HALF, 0, shift)
        later = lane >= shift
        zero = jnp.zeros((RC, HALF), F32)
        for c in range(2):
            for r in range(0, FULL, RC):
                rr = pl.ds(r, RC)
                r0 = pltpu.roll(win[c, rr, pl.ds(0, HALF)], fwd, axis=1)
                r1 = pltpu.roll(win[c, rr, pl.ds(HALF, HALF)], fwd, axis=1)
                vals = (jnp.where(later, r0, zero), jnp.where(later, r1, r0), jnp.where(later, zero, r1))
                for b in range(3):
                    acc[q + b, c, pl.ds(top + r, RC), :] = acc[q + b, c, pl.ds(top + r, RC), :] + vals[b]
        return carry

    @pl.when(d == 0)
    def _():
        lax.fori_loop(0, 2, lambda pos, carry: position(True, pos, carry), 0)

    @pl.when(d != 0)
    def _():
        lax.fori_loop(0, 2, lambda pos, carry: position(False, pos, carry), 0)

    for blk, out in ((0, g_on), (1, g_o), (2, g_i), (3, g_in)):
        out[...] = acc[blk + odd * (3 - 2 * blk)]


def merge(a, b, ra, rb, out, buf, sem):
    odd = lax.axis_index("tile") % 2
    copies = []
    for c in range(2):
        buf[c, :, pl.ds(pl.multiple_of(odd * HALF, HALF), HALF)] = a[c] + ra[odd, c]
        buf[c, :, pl.ds(pl.multiple_of((1 - odd) * HALF, HALF), HALF)] = b[c] + rb[c]
        copies.append(pltpu.make_async_copy(buf.at[c], out.at[0, c], sem.at[c]))
        copies[-1].start()
    for copy in copies:
        copy.wait()


def step(probe, object_slices, positions, measured):
    tiles = lax.axis_size("tile")
    cross = [(0, 3), (3, 0), (1, 2), (2, 1)]
    pair = [(i, i ^ 1) for i in range(tiles)]
    side = [(i, i + 1) for i in range(1, tiles - 1, 2)]
    side = side + [(j, i) for i, j in side]
    smem = pl.BlockSpec(memory_space=pltpu.SMEM)
    vmem = pl.BlockSpec(memory_space=pltpu.VMEM)
    anyw = pl.BlockSpec(memory_space=pltpu.HBM)
    block = pltpu.VMEM((2, ROWS, HALF), F32)
    own_o, own_i = pl.pallas_call(
        halve,
        out_shape=(block, block),
        in_specs=[anyw],
        out_specs=(vmem, vmem),
        scratch_shapes=[pltpu.SemaphoreType.DMA((2,))],
        name="halve",
        compiler_params=pltpu.CompilerParams(vmem_limit_bytes=2**20),
    )(in_hbm(object_slices))
    oth_o = lax.ppermute(own_o, ("depth", "mode"), cross)
    oth_i = lax.ppermute(own_i, ("depth", "mode"), cross)
    own_on = lax.ppermute(own_o, "tile", side)
    own_in = lax.ppermute(own_i, "tile", pair)
    prb = lax.ppermute(probe, "mode", [(0, 1), (1, 0)])
    oth_on = lax.ppermute(oth_o, "tile", side)
    oth_in = lax.ppermute(oth_i, "tile", pair)
    high, low, sort = (jnp.asarray(x) for x in tables())
    limit = pltpu.CompilerParams(vmem_limit_bytes=LIMIT)
    pair_of = pltpu.VMEM((2, 2, FULL, FULL), F32)
    info, mp, kh, kl, p0 = pl.pallas_call(
        prepare,
        out_shape=(pltpu.SMEM((2, 2), jnp.int32), pltpu.VMEM((2, 2, HALF, FULL), F32), pltpu.VMEM(high.shape, BF16),
                   pltpu.VMEM(low.shape, BF16), pltpu.VMEM((2, FULL, FULL), F32)),
        in_specs=[smem] + [anyw] * 5,
        out_specs=(smem,) + (vmem,) * 4,
        scratch_shapes=[
            pltpu.VMEM((2, FULL, HALF), F32),
            pltpu.VMEM((2, FULL, FULL), F32),
            pltpu.VMEM((FULL, FULL), BF16),
            pltpu.SemaphoreType.DMA((5,)),
        ],
        name="prepare",
        compiler_params=limit,
    )(positions, *map(in_hbm, (probe, measured, high, low, sort)))
    info = pltpu.with_memory_space_constraint(info, pltpu.SMEM)
    p0, p1, kh, kl, mp = map(in_vmem, (p0, prb[0], kh, kl, mp))
    fields = [pltpu.VMEM((2, 2, 2, FULL, FULL), BF16)] * 2 + [pair_of] * 2
    wown, psi = pl.pallas_call(
        early,
        out_shape=(pair_of, pltpu.VMEM((2, 2, 2, FULL, FULL), F32)),
        in_specs=[smem] + [vmem] * 8,
        out_specs=(vmem,) * 2,
        scratch_shapes=[pltpu.VMEM((4, 2, ROWS, HALF), F32)] + fields,
        name="early",
        compiler_params=limit,
    )(info, *map(in_vmem, (own_o, own_i, own_on, own_in)), p0, p1, kh, kl)
    g_o, g_i, g_on, g_in = pl.pallas_call(
        grad,
        out_shape=(block,) * 4,
        in_specs=[smem] + [vmem] * 11,
        out_specs=(vmem,) * 4,
        scratch_shapes=[
            pltpu.VMEM((4, 2, ROWS, HALF), F32),
            pltpu.VMEM((4, 2, ROWS, HALF), F32),
            pltpu.VMEM((2, FULL, FULL), F32),
            pair_of,
        ] + fields,
        name="grad",
        compiler_params=limit,
    )(info, *map(in_vmem, (oth_o, oth_i, oth_on, oth_in, wown, psi)), mp, p0, p1, kh, kl)
    groups = [[m * tiles + i, m * tiles + i + 1] for m in range(2) for i in range(1, tiles - 1, 2)]
    groups = groups + [[i, tiles + i] for i in (0, tiles - 1)]
    r_i = lax.ppermute(g_in, "tile", pair)
    r_o = lax.all_gather(g_on, ("mode", "tile"), axis_index_groups=groups)
    return pl.pallas_call(
        merge,
        out_shape=jax.ShapeDtypeStruct((1, 2, ROWS, FULL), F32),
        in_specs=[vmem] * 4,
        out_specs=anyw,
        scratch_shapes=[pltpu.VMEM((2, ROWS, FULL), F32), pltpu.SemaphoreType.DMA((2,))],
        name="merge",
        compiler_params=pltpu.CompilerParams(vmem_limit_bytes=LIMIT),
    )(*map(in_vmem, (g_o, g_i, r_o, r_i)))


def in_hbm(x):
    return pltpu.with_memory_space_constraint(x, pltpu.HBM)


def in_vmem(x):
    return pltpu.with_memory_space_constraint(x, pltpu.VMEM)


def solution(mesh):
    placed = (
        P("mode", None, None, None),
        P("depth", None, None, "tile"),
        P("tile", None),
        P("tile", None, None),
    )
    return jax.shard_map(step, mesh=mesh, in_specs=placed, out_specs=P("depth", None, None, "tile"), check_vma=False)
```
